32 devices in a mesh: tp: 4 (over z), dp: 8 (over y, x, core).
Axes of the slice: x: 2, y: 2, z: 4, core: 2. Of those that a mesh axis runs over, the one named last changes fastest.
Arguments:
- w_in: float32 [1, 1408, 10368], P(None, None, 'tp')
- w_out: float32 [1, 7552, 1408], P(None, 'tp')
- g_in: float32 [8, 1, 1408, 10368], P('dp', None, None, 'tp')
- g_out: float32 [8, 1, 7552, 1408], P('dp', None, 'tp')
- m_in: bfloat16 [1, 1408, 10368], P(None, 'dp', 'tp')
- m_out: bfloat16 [1, 7552, 1408], P(None, 'tp', 'dp')
- r_in: float32 [1, 1408], P(None, 'dp')
- c_in: float32 [1, 10368], P(None, 'tp')
- r_out: float32 [1, 7552], P(None, 'tp')
- c_out: float32 [1, 1408], P(None, 'dp')
- learn_rate: float32 [], replicated
- weight_decay: float32 [], replicated
- beta_two: float32 [], replicated
Outputs:
- output 1: float32 [1, 1408, 10368], P(None, None, 'tp')
- output 2: float32 [1, 7552, 1408], P(None, 'tp')
- output 3: bfloat16 [1, 1408, 10368], P(None, 'dp', 'tp')
- output 4: bfloat16 [1, 7552, 1408], P(None, 'tp', 'dp')
- output 5: float32 [1, 1408], P(None, 'dp')
- output 6: float32 [1, 10368], P(None, 'tp')
- output 7: float32 [1, 7552], P(None, 'tp')
- output 8: float32 [1, 1408], P(None, 'dp')
All inputs are finite; a program needn't handle non-finite values.
Results may differ from the reference program's by a relative error of at most 0.00125668.
Values sent between devices are 32-bit elements.
A program may use at most 1 GiB of HBM per device.

```python
import math
import jax
import jax.numpy as jnp

LAYERS = 1
D = 1408
MLP = 6144
DP = 8

FIN = MLP + 3 * D
FOUT = MLP + D


def axis_scales(key, count):
    key_ramp, key_noise = jax.random.split(key)
    ramp_slope = jax.random.uniform(key_ramp, (LAYERS, 1), jnp.float32, 0.6, 1.0)
    ramp_vals = jnp.linspace(-1.0, 1.0, count, dtype=jnp.float32)[None, :]
    noise_vals = jax.random.normal(key_noise, (LAYERS, count), jnp.float32)
    return jnp.exp(ramp_slope * ramp_vals + 0.3 * noise_vals)


def draw_matrix(key, n_rows, n_cols):
    key_list = jax.random.split(key, 7)
    row_scale = axis_scales(key_list[0], n_rows)
    col_scale = axis_scales(key_list[1], n_cols)
    noise_rep = jax.random.normal(key_list[2], (DP, LAYERS, n_rows, n_cols), jnp.float32)
    grad_rep = noise_rep * (row_scale[:, :, None] * col_scale[:, None, :] / math.sqrt(DP))
    grad_sum = jnp.sum(grad_rep, axis=0)
    grad_sq = grad_sum * grad_sum
    row_noise = jax.random.normal(key_list[3], (LAYERS, n_rows), jnp.float32)
    col_noise = jax.random.normal(key_list[4], (LAYERS, n_cols), jnp.float32)
    row_old = 0.25 * jnp.mean(grad_sq, axis=2) * jnp.exp(0.5 * row_noise)
    col_old = 0.25 * jnp.mean(grad_sq, axis=1) * jnp.exp(0.5 * col_noise)
    weight = jax.random.normal(key_list[5], (LAYERS, n_rows, n_cols), jnp.float32) * n_rows ** -0.5
    moment = (0.1 * jax.random.normal(key_list[6], (LAYERS, n_rows, n_cols), jnp.float32)).astype(jnp.bfloat16)
    return weight, grad_rep, moment, row_old, col_old


def setup_inputs(seed: int = 0) -> dict:
    key_list = jax.random.split(jax.random.key(seed), 5)
    w_in, g_in, m_in, r_in, c_in = draw_matrix(key_list[0], D, FIN)
    w_out, g_out, m_out, r_out, c_out = draw_matrix(key_list[1], FOUT, D)
    learn_rate = jax.random.uniform(key_list[2], (), jnp.float32, 0.25, 0.75) * D ** -0.5
    weight_decay = jax.random.uniform(key_list[3], (), jnp.float32, 0.15, 0.45) * D ** 0.5
    beta_two = jax.random.uniform(key_list[4], (), jnp.float32, 0.8, 0.9)
    return dict(w_in=w_in, w_out=w_out, g_in=g_in, g_out=g_out, m_in=m_in, m_out=m_out, r_in=r_in, c_in=c_in, r_out=r_out, c_out=c_out, learn_rate=learn_rate, weight_decay=weight_decay, beta_two=beta_two)


def adafactor_matrix(weight, grad_rep, moment, row_old, col_old, learn_rate, weight_decay, beta_two):
    grad_sum = jnp.sum(grad_rep, axis=0)
    grad_sq = grad_sum * grad_sum + 1e-30
    row_new = beta_two * row_old + (1.0 - beta_two) * jnp.mean(grad_sq, axis=2)
    col_new = beta_two * col_old + (1.0 - beta_two) * jnp.mean(grad_sq, axis=1)
    row_avg = jnp.mean(row_new, axis=1)
    second = row_new[:, :, None] * col_new[:, None, :] / row_avg[:, None, None]
    update = grad_sum / jnp.sqrt(second)
    rms_val = jnp.sqrt(jnp.mean(update * update, axis=(1, 2)))
    update = update / jnp.maximum(1.0, rms_val)[:, None, None]
    mom_new = (0.9 * moment.astype(jnp.float32) + 0.1 * update).astype(jnp.bfloat16)
    w_new = weight - learn_rate * mom_new.astype(jnp.float32) - learn_rate * weight_decay * weight
    return w_new, mom_new, row_new, col_new


def reference(w_in, w_out, g_in, g_out, m_in, m_out, r_in, c_in, r_out, c_out, learn_rate, weight_decay, beta_two):
    in_result = adafactor_matrix(w_in, g_in, m_in, r_in, c_in, learn_rate, weight_decay, beta_two)
    out_result = adafactor_matrix(w_out, g_out, m_out, r_out, c_out, learn_rate, weight_decay, beta_two)
    return (in_result[0], out_result[0], in_result[1], out_result[1], in_result[2], in_result[3], out_result[2], out_result[3])
```

```python
import functools
import jax
import jax.numpy as jnp
from jax import lax
from jax.experimental import pallas as pl
from jax.experimental.pallas import tpu as pltpu
from jax.sharding import PartitionSpec as P

F32 = jnp.float32
MESH = pl.DeviceIdType.MESH


def row_cuts(half):
    cuts, at = [], 0
    step = max(8, (half // 3 + 7) // 8 * 8)
    while at < half:
        cuts.append((at, min(step, half - at)))
        at += step
    return cuts


def lane_cuts(lanes, tiles):
    return [(at, min(tiles * 128, lanes - at)) for at in range(0, lanes, tiles * 128)]


def kernel(dims, lr_ref, wd_ref, b2_ref, w_in, w_out, g_in, g_out, m_in, m_out, r_in, c_in, r_out, c_out,
           w_in_new, w_out_new, m_in_new, m_out_new, r_in_new, c_in_new, r_out_new, c_out_new,
           acc_a, sib_a, one_a, two_a, wown, mom_a, acc_b, sib_b, one_b, two_b, stage, mom_b, momt_b,
           col_a, col_b, av_a, av_b, bv_a, bv_b, rb_a, rb_b, sd_a, sd_b, st_a, st_b,
           s_load, s_stage, s_misc, d_send_a, d_recv_a, d_send_b, d_recv_b, i_send_a, i_recv_a, i_send_b, i_recv_b,
           x_send_a, x_recv_a, x_send_b, x_recv_b, y_send_a, y_recv_a, y_send_b, y_recv_b, o_sem, q_send, q_recv):
    depth, lanes_a, rows_b, lanes_b, n_tp = dims
    ch = depth // 8
    half = ch // 2
    tp = lax.axis_index('tp')
    dp = lax.axis_index('dp')
    core = dp % 2
    chip = dp // 2
    chip_x = chip + 1 - 2 * (chip % 2)
    chip_y = chip + 2 - 4 * (chip // 2)
    chip_d = 3 - chip
    sib = dp + 1 - 2 * core
    dev_x = 2 * chip_x + core
    dev_y = 2 * chip_y + core
    sets = ((0, chip_x, dev_x, chip_y, dev_y), (half, chip_y, dev_y, chip_x, dev_x))
    cuts = row_cuts(half)
    n_cut = len(cuts)
    order = [[chip_d, chip_x, chip_y, chip], [chip_d, chip_y, chip_x, chip]]

    def remote(src, dst, ssem, rsem, dev):
        return pltpu.make_async_remote_copy(src_ref=src, dst_ref=dst, send_sem=ssem, recv_sem=rsem,
                                            device_id={'dp': dev}, device_id_type=MESH)

    def remote_tp(src, dst, ssem, rsem, dev):
        return pltpu.make_async_remote_copy(src_ref=src, dst_ref=dst, send_sem=ssem, recv_sem=rsem,
                                            device_id={'tp': dev}, device_id_type=MESH)

    def load_a(st, u):
        h0 = sets[st][0]
        slot = order[st][u]
        return pltpu.make_async_copy(g_in.at[pl.ds((2 * slot + core) * ch + h0, half)],
                                     acc_a.at[slot, pl.ds(h0, half)], s_load.at[st * 4 + u])

    for u in range(4):
        for st in range(2):
            load_a(st, u).start()
    blocks = lane_cuts(rows_b, 1)
    n_stage = stage.shape[0]

    def load_stage(src, j):
        at, num = blocks[j]
        return pltpu.make_async_copy(src.at[pl.ds(at, num)], stage.at[j % n_stage, pl.ds(0, num)], s_stage.at[j % n_stage])

    for j in range(min(n_stage, len(blocks))):
        load_stage(g_out, j).start()
    ld_w = pltpu.make_async_copy(w_in.at[pl.ds(dp * ch, ch)], wown, s_misc.at[0])
    ld_ma = pltpu.make_async_copy(m_in, mom_a, s_misc.at[1])
    ld_mb = pltpu.make_async_copy(m_out, mom_b.at[pl.ds(0, rows_b)], s_misc.at[2])

    barrier = pltpu.get_barrier_semaphore()
    for d in range(1, 8):
        pl.semaphore_signal(barrier, inc=1, device_id={'dp': (dp + d) % 8}, device_id_type=MESH)
    for d in range(1, n_tp):
        pl.semaphore_signal(barrier, inc=1, device_id={'tp': (tp + d) % n_tp}, device_id_type=MESH)
    pl.semaphore_wait(barrier, 7 + n_tp - 1)

    def d2d_a(st, u, c, other):
        h0 = sets[st][0]
        slot = order[st][u]
        at, num = cuts[c]
        i = (st * 4 + u) * n_cut + c
        return remote(g_in.at[pl.ds((2 * slot + 1 - core) * ch + h0 + at, num)],
                      sib_a.at[slot, pl.ds(h0 + at, num)], d_send_a.at[i], d_recv_a.at[i], sib)

    def d2d_b(st, u, other):
        h0 = sets[st][0]
        slot = order[st][u]
        i = st * 4 + u
        return remote(acc_b.at[pl.ds((2 * slot + 1 - core) * ch + h0, half)],
                      sib_b.at[slot, pl.ds(h0, half)], d_send_b.at[i], d_recv_b.at[i], sib)

    for u in range(4):
        for c in range(n_cut):
            for st in range(2):
                d2d_a(st, u, c, True).start()
    ld_w.start()
    ld_ma.start()
    ld_mb.start()

    def view_a(slot, r0, num):
        return acc_a.at[slot, pl.ds(r0, num)]

    def view_b(slot, r0, num):
        return acc_b.at[pl.ds((2 * slot + core) * ch + r0, num)]

    def add(dst, src, num):
        def step(i, carry):
            r = pl.ds(pl.multiple_of(i * 8, 8), 8)
            dst[r, :] = dst[r, :] + src[r, :]
            return carry
        lax.fori_loop(0, num // 8, step, 0)

    class Mat:
        pass

    a, b = Mat(), Mat()
    a.view, a.one, a.two, a.isend, a.irecv, a.sibling = view_a, one_a, two_a, i_send_a, i_recv_a, sib_a
    b.view, b.one, b.two, b.isend, b.irecv, b.sibling = view_b, one_b, two_b, i_send_b, i_recv_b, sib_b

    def hop(m, st, u, c):
        h0, c1, dev1, c2, dev2 = sets[st]
        at, num = cuts[c]
        i = (st * 3 + u) * n_cut + c
        if u == 0:
            src, dst, dev = m.view(chip_d, h0 + at, num), m.one.at[st, 0, pl.ds(at, num)], dev1
        elif u == 1:
            src, dst, dev = m.view(c1, h0 + at, num), m.one.at[st, 1, pl.ds(at, num)], dev1
        else:
            src, dst, dev = m.view(c2, h0 + at, num), m.two.at[st, pl.ds(at, num)], dev2
        return remote(src, dst, m.isend.at[i], m.irecv.at[i], dev)

    def pair_up(m, st, u, c):
        h0 = sets[st][0]
        slot = order[st][u]
        at, num = cuts[c]
        if m is a:
            if c == 0:
                load_a(st, u).wait()
            d2d_a(st, u, c, False).wait_recv()
        elif c == 0:
            d2d_b(st, u, False).wait_recv()
        add(m.view(slot, h0 + at, num), m.sibling.at[slot, pl.ds(h0 + at, num)], num)

    def first(m, u):
        for c in range(n_cut):
            for st in range(2):
                pair_up(m, st, u, c)
            for st in range(2):
                hop(m, st, u, c).start()

    def settle(m):
        for u in (2, 3):
            for c in range(n_cut):
                for st in range(2):
                    pair_up(m, st, u, c)

    def second(m):
        for c in range(n_cut):
            at, num = cuts[c]
            for st in range(2):
                hop(m, st, 0, c).wait_recv()
                add(m.view(sets[st][3], sets[st][0] + at, num), m.one.at[st, 0, pl.ds(at, num)], num)
            for st in range(2):
                hop(m, st, 2, c).start()

    def finish(m):
        for u, buf in ((1, m.one), (2, m.two)):
            for c in range(n_cut):
                at, num = cuts[c]
                for st in range(2):
                    hop(m, st, u, c).wait_recv()
                    src = m.one.at[st, 1, pl.ds(at, num)] if u == 1 else m.two.at[st, pl.ds(at, num)]
                    add(m.view(chip, sets[st][0] + at, num), src, num)
        for u in range(3):
            for c in range(n_cut):
                for st in range(2):
                    hop(m, st, u, c).wait_send()
        for u in range(4):
            for st in range(2):
                if m is a:
                    for c in range(n_cut):
                        d2d_a(st, u, c, True).wait_send()
                else:
                    d2d_b(st, u, True).wait_send()

    def transpose_b():
        for j, (at, num) in enumerate(blocks):
            load_stage(g_out, j).wait()
            buf = stage.at[j % n_stage]
            if num < 128:
                buf[num:, :] = jnp.zeros((128 - num, depth), F32)
            acc_b[:, at:at + 128] = buf[...].T
            if j + n_stage < len(blocks):
                load_stage(g_out, j + n_stage).start()
        for u in range(4):
            for st in range(2):
                d2d_b(st, u, True).start()

    n_in, n_out = lanes_a * n_tp, rows_b * n_tp
    beta = b2_ref[0]
    a.lanes, a.valid, a.col, a.av, a.bv, a.rb, a.sd, a.st = lanes_a, lanes_a, col_a, av_a, bv_a, rb_a, sd_a, st_a
    b.lanes, b.valid, b.col, b.av, b.bv, b.rb, b.sd, b.st = lanes_b, rows_b, col_b, av_b, bv_b, rb_b, sd_b, st_b
    a.aold, a.bold, a.anew, a.bnew, a.na, a.nb, a.q = r_in, c_in, r_in_new, c_in_new, n_in, depth, 0
    b.aold, b.bold, b.anew, b.bnew, b.na, b.nb, b.q = c_out, r_out, c_out_new, r_out_new, n_out, depth, 20
    eye = lax.broadcasted_iota(jnp.int32, (ch, ch), 0) == lax.broadcasted_iota(jnp.int32, (ch, ch), 1)

    def all_dp(m, buf, base):
        return [remote(buf.at[dp], buf.at[dp], q_send.at[m.q + base + d - 1], q_recv.at[m.q + base + d - 1], (dp + d) % 8)
                for d in range(1, 8)]

    def all_tp(m, buf, base):
        return [remote_tp(buf.at[tp], buf.at[tp], q_send.at[m.q + base + d - 1], q_recv.at[m.q + base + d - 1], (tp + d) % n_tp)
                for d in range(1, n_tp)]

    def wait_dp(m, buf, base):
        for d in range(1, 8):
            src = (dp + 8 - d) % 8
            cp = remote(buf.at[src], buf.at[src], q_send.at[m.q + base + d - 1], q_recv.at[m.q + base + d - 1], src)
            cp.wait_recv()
            cp.wait_send()

    def wait_tp(m, buf, base):
        for d in range(1, n_tp):
            src = (tp + n_tp - d) % n_tp
            cp = remote_tp(buf.at[src], buf.at[src], q_send.at[m.q + base + d - 1], q_recv.at[m.q + base + d - 1], src)
            cp.wait_recv()
            cp.wait_send()

    def stat1(m):
        own = m.view(chip, 0, ch)
        eps = jnp.full((1, m.lanes), 1e-30, F32)
        if m.valid < m.lanes:
            eps = jnp.where(lax.broadcasted_iota(jnp.int32, (1, m.lanes), 1) < m.valid, eps, 0.0)

        def step(i, colsum):
            r = pl.ds(pl.multiple_of(i * 8, 8), 8)
            g = own[r, :]
            sq = g * g + eps
            m.col[r, :] = jnp.broadcast_to(jnp.sum(sq, axis=1, keepdims=True), (8, 128))
            return colsum + sq
        colsum = lax.fori_loop(0, ch // 8, step, jnp.zeros((8, m.lanes), F32))
        m.bv[dp] = jnp.sum(colsum, axis=0, keepdims=True)
        rows = jnp.broadcast_to(m.col[:, 0:1], (ch, ch))
        m.av[tp] = jnp.sum(jnp.where(eye, rows, 0.0), axis=0, keepdims=True)
        for cp in all_dp(m, m.bv, 0) + all_tp(m, m.av, 7):
            cp.start()

    def stat2(m):
        own = m.view(chip, 0, ch)
        wait_dp(m, m.bv, 0)
        wait_tp(m, m.av, 7)
        bsum = m.bv[0]
        for i in range(1, 8):
            bsum = bsum + m.bv[i]
        asum = m.av[0]
        for i in range(1, n_tp):
            asum = asum + m.av[i]
        anew = beta * m.aold[...] + (1.0 - beta) * (asum / m.na)
        bnew = beta * m.bold[...] + (1.0 - beta) * (bsum[:, :m.valid] / m.nb)
        m.anew[...] = anew
        m.bnew[...] = bnew
        if m.valid < m.lanes:
            m.rb[...] = jnp.zeros((8, m.lanes), F32)
        m.rb[:, :m.valid] = jnp.broadcast_to(1.0 / jnp.sqrt(bnew), (8, m.valid))
        ra = 1.0 / jnp.sqrt(anew)
        m.col[...] = jnp.broadcast_to(
            jnp.sum(jnp.where(eye, jnp.broadcast_to(ra, (ch, ch)), 0.0), axis=1, keepdims=True), (ch, 128))

        def step(i, total):
            r = pl.ds(pl.multiple_of(i * 8, 8), 8)
            t = own[r, :] * m.col[r, 0:1] * m.rb[...]
            own[r, :] = t
            return total + t * t
        total = lax.fori_loop(0, ch // 8, step, jnp.zeros((8, m.lanes), F32))
        total = jnp.sum(jnp.sum(total, axis=1, keepdims=True), axis=0, keepdims=True)
        rsum = jnp.sum(anew if m is a else bnew, axis=1, keepdims=True)
        lane = lax.broadcasted_iota(jnp.int32, (1, 128), 1)
        m.sd[dp] = jnp.where(lane == 0, jnp.broadcast_to(total, (1, 128)), jnp.broadcast_to(rsum, (1, 128)))
        for cp in all_dp(m, m.sd, 10):
            cp.start()

    def stat3(m):
        mine = m.sd[dp]
        wait_dp(m, m.sd, 10)
        tot = m.sd[0]
        for i in range(1, 8):
            tot = tot + m.sd[i]
        if m is b:
            lane = lax.broadcasted_iota(jnp.int32, (1, 128), 1)
            tot = jnp.where(lane == 0, tot, mine)
        m.st[tp] = tot
        for cp in all_tp(m, m.st, 17):
            cp.start()

    def factor(m):
        wait_tp(m, m.st, 17)
        mine = m.st[tp]
        tot = m.st[0]
        for i in range(1, n_tp):
            tot = tot + m.st[i]
        usum = tot[:, 0:1]
        if m is a:
            ravg = mine[:, 1:2] / depth
            count = depth * n_in
        else:
            ravg = tot[:, 1:2] / n_out
            count = depth * n_out
        rms = jnp.sqrt(ravg * usum / count)
        return jnp.sqrt(ravg) / jnp.maximum(1.0, rms)

    lr = lr_ref[0]
    decay = lr_ref[0] * wd_ref[0]

    new_a = sib_a

    def out_a(slot, r0, num, own_core):
        k = core if own_core else 1 - core
        return w_in_new.at[pl.ds((2 * slot + k) * ch + r0, num)]

    def ring(st, u, send):
        h0, c1, dev1, c2, dev2 = sets[st]
        if send:
            return (chip, dev2) if u == 0 else (chip, dev1) if u == 1 else (c2, dev1)
        return (c2, dev2) if u == 0 else (c1, dev1) if u == 1 else (chip_d, dev1)

    def x_a(st, u, c, send):
        slot, dev = ring(st, u, send)
        at, num = cuts[c]
        i = (st * 3 + u) * n_cut + c
        ref = new_a.at[slot, pl.ds(sets[st][0] + at, num)]
        return remote(ref, ref, x_send_a.at[i], x_recv_a.at[i], dev)

    def y_a(st, u, c, send):
        slot = order[st][u]
        at, num = cuts[c]
        i = (st * 4 + u) * n_cut + c
        r0 = sets[st][0] + at
        src = new_a.at[slot, pl.ds(r0, num)]
        return remote(src, out_a(slot, r0, num, send), y_send_a.at[i], y_recv_a.at[i], sib)

    def o_a(st, u, c):
        slot = order[st][u]
        at, num = cuts[c]
        i = (st * 4 + u) * n_cut + c
        r0 = sets[st][0] + at
        return pltpu.make_async_copy(new_a.at[slot, pl.ds(r0, num)], out_a(slot, r0, num, True), o_sem.at[i])

    def emit_a(st, u, c):
        y_a(st, u, c, True).start()
        o_a(st, u, c).start()

    def final_a():
        f = factor(a)
        own = view_a(chip, 0, ch)
        ld_w.wait()
        ld_ma.wait()

        def step(i, carry):
            r = pl.ds(pl.multiple_of(i * 16, 16), 16)
            u = own[r, :] * f
            mom = (0.9 * mom_a[r, :].astype(F32) + 0.1 * u).astype(jnp.bfloat16)
            mom_a[r, :] = mom
            w = wown[r, :]
            new_a[chip, r, :] = w - lr * mom.astype(F32) - decay * w
            return carry
        lax.fori_loop(0, ch // 16, step, 0)
        pltpu.make_async_copy(mom_a, m_in_new, s_misc.at[1]).start()

    def own_a(c):
        for st in range(2):
            x_a(st, 0, c, True).start()
        for st in range(2):
            x_a(st, 1, c, True).start()
        for st in range(2):
            emit_a(st, 3, c)

    def forward_a(c):
        for st in range(2):
            x_a(st, 0, c, False).wait_recv()
            x_a(st, 2, c, True).start()
            emit_a(st, 2, c)
        for st in range(2):
            x_a(st, 1, c, False).wait_recv()
            emit_a(st, 1, c)

    def last_a(c):
        for st in range(2):
            x_a(st, 2, c, False).wait_recv()
            emit_a(st, 0, c)

    def drain_a():
        for c in range(n_cut):
            for st in range(2):
                for u in range(3):
                    x_a(st, u, c, True).wait_send()
                for u in range(4):
                    y_a(st, u, c, True).wait_send()
                    y_a(st, u, c, False).wait_recv()
                    o_a(st, u, c).wait()
        pltpu.make_async_copy(mom_a, m_in_new, s_misc.at[1]).wait()

    parts = lane_cuts(lanes_b, 3)
    n_part = len(parts)

    def x_b(st, u, c, send):
        slot, dev = ring(st, u, send)
        at, num = parts[c]
        i = (st * 3 + u) * n_part + c
        ref = acc_b.at[pl.ds((2 * slot + core) * ch + sets[st][0], half), pl.ds(at, num)]
        return remote(ref, ref, x_send_b.at[i], x_recv_b.at[i], dev)

    def y_b(st, u, c, send):
        slot = order[st][u]
        at, num = parts[c]
        i = (st * 4 + u) * n_part + c
        k = core if send else 1 - core
        ref = acc_b.at[pl.ds((2 * slot + k) * ch + sets[st][0], half), pl.ds(at, num)]
        return remote(ref, ref, y_send_b.at[i], y_recv_b.at[i], sib)

    def moment_b():
        ld_mb.wait()
        if len(blocks) * 128 > rows_b:
            mom_b[rows_b:, :] = jnp.zeros((len(blocks) * 128 - rows_b, ch), jnp.bfloat16)
        for j in range(len(blocks)):
            momt_b[:, j * 128:j * 128 + 128] = mom_b[j * 128:j * 128 + 128, :].astype(F32).T

    def final_b():
        f = factor(b)
        own = view_b(chip, 0, ch)

        def step(i, carry):
            r = pl.ds(pl.multiple_of(i * 8, 8), 8)
            u = own[r, :] * f
            own[r, :] = (0.9 * momt_b[r, :] + 0.1 * u).astype(jnp.bfloat16).astype(F32)
            return carry
        lax.fori_loop(0, ch // 8, step, 0)

    def store_moment_b():
        own = view_b(chip, 0, ch)
        for j in range(len(blocks)):
            mom_b[j * 128:j * 128 + 128, :] = own[:, j * 128:j * 128 + 128].T.astype(jnp.bfloat16)
        pltpu.make_async_copy(mom_b.at[pl.ds(0, rows_b)], m_out_new, s_misc.at[2]).start()

    def own_b(c):
        for st in range(2):
            x_b(st, 0, c, True).start()
        for st in range(2):
            x_b(st, 1, c, True).start()
        for st in range(2):
            y_b(st, 3, c, True).start()

    def forward_b(c):
        for st in range(2):
            x_b(st, 0, c, False).wait_recv()
            x_b(st, 2, c, True).start()
            y_b(st, 2, c, True).start()
        for st in range(2):
            x_b(st, 1, c, False).wait_recv()
            y_b(st, 1, c, True).start()

    def last_b(c):
        for st in range(2):
            x_b(st, 2, c, False).wait_recv()
            y_b(st, 0, c, True).start()

    def put_b(j):
        at, num = blocks[j]
        return pltpu.make_async_copy(stage.at[j % n_stage, pl.ds(0, num)], w_out_new.at[pl.ds(at, num)], s_stage.at[n_stage + j % n_stage])

    def finish_b(c):
        for st in range(2):
            for u in range(4):
                y_b(st, u, c, False).wait_recv()
        at, num = parts[c]
        for j in range(at // 128, (at + num) // 128):
            load_stage(w_out, j).wait()
            buf = stage.at[j % n_stage]
            w = buf[...]
            buf[...] = w - lr * acc_b[:, j * 128:j * 128 + 128].T - decay * w
            put_b(j).start()
            nxt = j - 1 + n_stage
            if j >= 1 and nxt < len(blocks):
                put_b(j - 1).wait()
                load_stage(w_out, nxt).start()

    def drain_b():
        for c in range(n_part):
            for st in range(2):
                for u in range(3):
                    x_b(st, u, c, True).wait_send()
                for u in range(4):
                    y_b(st, u, c, True).wait_send()
        for j in range(max(0, len(blocks) - n_stage), len(blocks)):
            put_b(j).wait()
        pltpu.make_async_copy(mom_b.at[pl.ds(0, rows_b)], m_out_new, s_misc.at[2]).wait()

    first(a, 0)
    first(a, 1)
    settle(a)
    transpose_b()
    second(a)
    first(b, 0)
    moment_b()
    finish(a)
    stat1(a)
    first(b, 1)
    settle(b)
    stat2(a)
    second(b)
    stat3(a)
    final_a()
    own_a(0)
    finish(b)
    stat1(b)
    for c in range(1, n_cut):
        own_a(c)
        forward_a(c - 1)
        if c == 1:
            stat2(b)
        if c >= 2:
            last_a(c - 2)
    for j in range(min(n_stage, len(blocks))):
        load_stage(w_out, j).start()
    stat3(b)
    forward_a(n_cut - 1)
    if n_cut >= 2:
        last_a(n_cut - 2)
    final_b()
    own_b(0)
    last_a(n_cut - 1)
    store_moment_b()
    for c in range(1, n_part + 3):
        if c < n_part:
            own_b(c)
        if 0 <= c - 1 < n_part:
            forward_b(c - 1)
        if 0 <= c - 2 < n_part:
            last_b(c - 2)
        if 0 <= c - 3 < n_part:
            finish_b(c - 3)
    drain_a()
    drain_b()


def fused(dims, args):
    depth, lanes_a, rows_b, lanes_b, n_tp = dims
    ch = depth // 8
    half = ch // 2
    n_cut = len(row_cuts(half))
    n_part = len(lane_cuts(lanes_b, 3))
    n_stage = 5
    any_spec = pl.BlockSpec(memory_space=pl.ANY)
    vec = pl.BlockSpec(memory_space=pltpu.VMEM)
    smem = pl.BlockSpec(memory_space=pltpu.SMEM)
    dma = pltpu.SemaphoreType.DMA
    sh = jax.ShapeDtypeStruct
    return pl.pallas_call(
        functools.partial(kernel, dims),
        out_shape=(sh((depth, lanes_a), F32), sh((rows_b, depth), F32), sh((ch, lanes_a), jnp.bfloat16),
                   sh((rows_b, ch), jnp.bfloat16), sh((1, ch), F32), sh((1, lanes_a), F32), sh((1, rows_b), F32), sh((1, ch), F32)),
        in_specs=[smem] * 3 + [any_spec] * 6 + [vec] * 4,
        out_specs=(any_spec,) * 4 + (vec,) * 4,
        scratch_shapes=[
            pltpu.VMEM((4, ch, lanes_a), F32), pltpu.VMEM((4, ch, lanes_a), F32),
            pltpu.VMEM((2, 2, half, lanes_a), F32), pltpu.VMEM((2, half, lanes_a), F32),
            pltpu.VMEM((ch, lanes_a), F32), pltpu.VMEM((ch, lanes_a), jnp.bfloat16),
            pltpu.VMEM((depth, lanes_b), F32), pltpu.VMEM((4, ch, lanes_b), F32),
            pltpu.VMEM((2, 2, half, lanes_b), F32), pltpu.VMEM((2, half, lanes_b), F32),
            pltpu.VMEM((n_stage, 128, depth), F32), pltpu.VMEM((lanes_b, ch), jnp.bfloat16), pltpu.VMEM((ch, lanes_b), F32),
            pltpu.VMEM((ch, 128), F32), pltpu.VMEM((ch, 128), F32),
            pltpu.VMEM((n_tp + 8, 1, ch), F32), pltpu.VMEM((n_tp + 8, 1, ch), F32),
            pltpu.VMEM((9, 1, lanes_a), F32), pltpu.VMEM((9, 1, lanes_b), F32),
            pltpu.VMEM((8, lanes_a), F32), pltpu.VMEM((8, lanes_b), F32),
            pltpu.VMEM((16, 1, 128), F32), pltpu.VMEM((16, 1, 128), F32),
            pltpu.VMEM((n_tp + 8, 1, 128), F32), pltpu.VMEM((n_tp + 8, 1, 128), F32),
            dma((8,)), dma((2 * n_stage,)), dma((3,)),
            dma((8 * n_cut,)), dma((8 * n_cut,)), dma((8,)), dma((8,)),
            dma((6 * n_cut,)), dma((6 * n_cut,)), dma((6 * n_cut,)), dma((6 * n_cut,)),
            dma((6 * n_cut,)), dma((6 * n_cut,)), dma((6 * n_part,)), dma((6 * n_part,)),
            dma((8 * n_cut,)), dma((8 * n_cut,)), dma((8 * n_part,)), dma((8 * n_part,)),
            dma((8 * n_cut,)), dma((40,)), dma((40,)),
        ],
        compiler_params=pltpu.CompilerParams(collective_id=0, has_side_effects=True, vmem_limit_bytes=66 * 1000 * 1000),
    )(*args)


def solution(mesh):
    n_tp = mesh.shape['tp']

    def body(w_in, w_out, g_in, g_out, m_in, m_out, r_in, c_in, r_out, c_out, learn_rate, weight_decay, beta_two):
        depth, lanes_a = w_in.shape[1:]
        rows_b = w_out.shape[1]
        dims = (depth, lanes_a, rows_b, (rows_b + 127) // 128 * 128, n_tp)
        outs = fused(dims, (learn_rate.reshape(1), weight_decay.reshape(1), beta_two.reshape(1), w_in[0], w_out[0],
                            g_in[0, 0], g_out[0, 0], m_in[0], m_out[0], r_in, c_in, r_out, c_out))
        return tuple(o[None] for o in outs[:4]) + tuple(outs[4:])

    in_specs = (P(None, None, 'tp'), P(None, 'tp', None), P('dp', None, None, 'tp'), P('dp', None, 'tp', None), P(None, 'dp', 'tp'), P(None, 'tp', 'dp'), P(None, 'dp'), P(None, 'tp'), P(None, 'tp'), P(None, 'dp'), P(), P(), P())
    out_specs = (P(None, None, 'tp'), P(None, 'tp', None), P(None, 'dp', 'tp'), P(None, 'tp', 'dp'), P(None, 'dp'), P(None, 'tp'), P(None, 'tp'), P(None, 'dp'))
    return jax.shard_map(body, mesh=mesh, in_specs=in_specs, out_specs=out_specs, check_vma=False)
```
